128 devices in a mesh: task: 8 (over x_hi, z), dp: 16 (over x_lo, y, core).
Axes of the slice: x: 4 (x_hi: 2, x_lo: 2; x = x_hi * 2 + x_lo), y: 4, z: 4, core: 2. Of those that a mesh axis runs over, the one named last changes fastest.
Arguments:
- tokens_in: bfloat16 [131072, 4096], P(('task', 'dp')), may hold values from -45 to 45
- query_cotangent: bfloat16 [131072, 2048], P(('task', 'dp')), may hold values from -23040 to 23040
- task_index: int32 [131072], P(('task', 'dp')), may hold values from 0 to 15, as said below
- loss_weights: int32 [16], replicated, may hold values from 1 to 4
- master: float32 [4096, 2048], P(('task', 'dp')), may hold values from -6 to 6
- moment_first: float32 [4096, 2048], P(('task', 'dp')), may hold values from -6 to 6
- moment_second: float32 [4096, 2048], P(('task', 'dp')), may hold values from 0.05 to 5
Outputs:
- new_master: float32 [4096, 2048], P(('task', 'dp'))
- new_first: float32 [4096, 2048], P(('task', 'dp'))
- new_second: float32 [4096, 2048], P(('task', 'dp'))
The draws below stay inside these ranges and needn't reach their ends.
Inputs may be any that keep to these rules, and one draw needn't show every extreme that they name: `task_index`: the first 16 tokens name each task once.
All inputs are finite; a program needn't handle non-finite values.
Results may differ from the reference program's by a relative error of at most 0.00042.
Values may be sent and summed in bfloat16 or wider, within the bound.
No kernel may reach another device: no remote copies, remote signals or barrier semaphores. Data moves between devices by JAX's collectives and lax.ppermute only.
A program may use at most 192 MiB of HBM per device.

```python
import math
import jax
import jax.numpy as jnp
from jax import lax

D = 4096
QW = 2048
TASKS = 16
TOK_DEV = 1024
TOKENS = 131072
DEVICES = 128


def column_profile(key, col_count, spread):
    position = jnp.arange(col_count, dtype=jnp.float32) / col_count
    exponent = jax.random.uniform(key, (col_count,), jnp.float32)
    return 3.0 ** position * spread ** exponent


def field_values(key, row_count, col_count):
    subkeys = jax.random.split(key, 2)
    scales = column_profile(subkeys[0], col_count, 10.0)
    values = jnp.clip(jax.random.normal(subkeys[1], (row_count, col_count), jnp.float32), -6.0, 6.0)
    return values * scales[None, :] * 0.25


def draw_tokens_in(key, part):
    return field_values(jax.random.fold_in(key, 11), TOKENS, D).astype(jnp.bfloat16)


def draw_query_cotangent(key, part):
    amplitude = float(TOKENS // (TASKS * TASKS))
    inputs = field_values(jax.random.fold_in(key, 11), TOKENS, D)
    own_part = field_values(jax.random.fold_in(key, 23), TOKENS, QW)
    block_size = math.gcd(QW, 128)
    block_count = QW // block_size
    mixing = jax.random.normal(jax.random.fold_in(key, 29), (block_count, block_size, block_size), jnp.float32)
    mixing = mixing / math.sqrt(block_size)
    leading = inputs[:, :QW].reshape(TOKENS, block_count, block_size)
    carried = jnp.einsum('nbk,bkj->nbj', leading, mixing, precision=lax.Precision.HIGHEST)
    combined = jnp.clip(own_part + 0.15 * carried.reshape(TOKENS, QW), -45.0, 45.0)
    return (combined * amplitude).astype(jnp.bfloat16)


def draw_task_index(key, part):
    subkeys = jax.random.split(jax.random.fold_in(key, 37), 2)
    rows_all = jnp.arange(TOKENS, dtype=jnp.int32)
    shifted = rows_all * TASKS // TOKENS
    offsets = jax.random.randint(subkeys[0], (TOKENS,), 0, TASKS // 2, dtype=jnp.int32)
    sliding = (shifted + offsets) % TASKS
    ordering = jax.random.permutation(subkeys[1], jnp.arange(TASKS, dtype=jnp.int32))
    leading = ordering[jnp.minimum(rows_all, TASKS - 1)]
    return jnp.where(rows_all < TASKS, leading, sliding).astype(jnp.int32)


def set_ends(result, key, least, high):
    index_at = [jax.random.randint(jax.random.fold_in(key, axis), (), 0, length) for axis, length in enumerate(result.shape)]
    main_axis = result.shape.index(max(result.shape))
    neighbour = index_at[:main_axis] + [(index_at[main_axis] + 1) % result.shape[main_axis]] + index_at[main_axis + 1:]
    return result.at[tuple(index_at)].set(least).at[tuple(neighbour)].set(high)


def level_of(key, dims, shards, low, high):
    loudness = 1.0
    for dim, shards_of in shards:
        draws = jax.random.uniform(jax.random.fold_in(jax.random.fold_in(key, 6), dim), (shards_of,), jnp.float32, low / len(shards), high / len(shards))
        loudness = loudness * jnp.repeat(jnp.exp(draws), dims[dim] // shards_of).reshape((-1,) + (1,) * (len(dims) - 1 - dim))
    return loudness


def normal_values(stream_key, extent, width, limit, pieces=(), held_as=jnp.bfloat16):
    level = level_of(stream_key, extent, pieces, -0.22, 0.18) if pieces else 1.0
    array = jax.random.normal(stream_key, extent, jnp.float32) * width * level
    return jnp.minimum(jnp.maximum(array, -limit), limit).astype(held_as)


def setup_inputs(seed: int = 0) -> dict:
    key_of = jax.random.split(jax.random.key(seed), 8)
    tokens_in = draw_tokens_in(jax.random.fold_in(key_of[7], 71), 0)
    query_cotangent = draw_query_cotangent(jax.random.fold_in(key_of[7], 71), 0)
    task_index = draw_task_index(jax.random.fold_in(key_of[7], 71), 0)
    loss_weights = set_ends(jax.random.randint(key_of[3], (TASKS,), 1, 5), jax.random.fold_in(key_of[3], 1), 1, 4).astype(jnp.int32)
    master = normal_values(key_of[4], (D, QW), 1.0, 6.0, ((0, 128),), jnp.float32)
    moment_first = normal_values(key_of[5], (D, QW), 1.0, 6.0, ((0, 128),), jnp.float32)
    moment_second = jnp.clip(jnp.exp(math.log(5.0) - 4.6051702 * jax.random.uniform(key_of[6], (D, QW), jnp.float32) ** level_of(key_of[6], (D, QW), ((0, 128),), -0.2, 0.2)), 0.05, 5.0)
    return dict(tokens_in=tokens_in, query_cotangent=query_cotangent, task_index=task_index, loss_weights=loss_weights, master=master, moment_first=moment_first, moment_second=moment_second)


beta_one = 0.9
beta_two = 0.95
adam_eps = 1e-08
step_rate = 0.01
decay_rate = 0.1
corr_one = 1.0 - 0.9 ** 10
corr_two = 1.0 - 0.95 ** 10

def reference(tokens_in, query_cotangent, task_index, loss_weights, master, moment_first, moment_second):
    labels = jnp.arange(TASKS, dtype=jnp.int32)
    member = task_index[:, None] == labels[None, :]
    counts = lax.optimization_barrier(jnp.sum(member.astype(jnp.int32), axis=0))
    task_scale = loss_weights.astype(jnp.float32) / counts.astype(jnp.float32)
    token_scale = lax.optimization_barrier(jnp.sum(jnp.where(member, task_scale[None, :], jnp.float32(0.0)), axis=1))
    weighted = (query_cotangent.astype(jnp.float32) * token_scale[:, None]).astype(jnp.bfloat16)
    token_blocks = tokens_in.reshape(DEVICES, TOK_DEV, D)
    weight_blocks = weighted.reshape(DEVICES, TOK_DEV, QW)

    def add_block(running, blocks_pair):
        product = jnp.dot(blocks_pair[0].T, blocks_pair[1], preferred_element_type=jnp.float32)
        return (running + product, None)
    gradient, unused = lax.scan(add_block, jnp.zeros((D, QW), jnp.float32), (token_blocks, weight_blocks))
    square_sum = jnp.sum(gradient * gradient)
    root_mean = jnp.sqrt(square_sum / (D * QW))
    clip = 1.0 / jnp.maximum(root_mean, 1.0)
    clipped = gradient * clip
    new_first = beta_one * moment_first + (1.0 - beta_one) * clipped
    new_second = beta_two * moment_second + (1.0 - beta_two) * clipped * clipped
    direction = new_first / corr_one / (jnp.sqrt(new_second / corr_two) + adam_eps)
    new_master = master - step_rate * (direction + decay_rate * master)
    return (new_master, new_first, new_second)
```

```python
import jax
import jax.numpy as jnp
from jax import lax
from jax.experimental import pallas as pl
from jax.experimental.pallas import tpu as pltpu
from jax.sharding import Mesh
from jax.sharding import PartitionSpec as P

D = 4096
QW = 2048
AXES = ("task_0", "task_1", "dp_0", "dp_1", "dp_2")
SIZES = (2, 4, 2, 4, 2)
DEVICES = 128
DOWN = 2.0**-11
UP = 2.0**11
HALF = QW // 2
WIDTHS = (384, 384, 256)
ORDERS = ("xyz", "yzx", "zxy")


beta_one = 0.9
beta_two = 0.95
adam_eps = 1e-08
step_rate = 0.01
decay_rate = 0.1
corr_one = 1.0 - 0.9**10
corr_two = 1.0 - 0.95**10


def coords(index):
    out = []
    for size in reversed(SIZES):
        out.append(index % size)
        index //= size
    return out[::-1]


def number(parts):
    index = 0
    for part, size in zip(parts, SIZES):
        index = index * size + part
    return index


def flipped(parts, axis, both):
    xh, z, xl, y, c = parts
    if axis == "x":
        return (xh ^ both, z, xl ^ 1, y, c)
    if axis == "y":
        return (xh, z, xl, y ^ (1 + 2 * both), c)
    if axis == "z":
        return (xh, z ^ (1 + 2 * both), xl, y, c)
    return (xh, z, xl, y, c ^ 1)


def swap(value, axis, step):
    pairs = []
    for index in range(DEVICES):
        parts = coords(index)
        both = parts[4] ^ step
        pairs.append((index, number(flipped(parts, axis, both))))
    return lax.ppermute(value, AXES, pairs)


def wide(value):
    return value.astype(jnp.float32)


def narrow(value):
    return value.astype(jnp.float16)


def total(value):
    spread = jnp.broadcast_to(value[None], (DEVICES, 1, 128))
    arrived = lax.all_to_all(spread, AXES, split_axis=0, concat_axis=0, tiled=True)
    return arrived.sum(axis=0)


def mirrored(s):
    return (s % 2) * 2 + s // 2


def laid_out(tokens_in, places, shuffle):
    count = tokens_in.shape[0]

    def kernel(place, x_ref, p_ref, xk, xs, pxk, pxs, yk, ys, pyk, pys, zk, zs, pzk, pzs):
        turned = lax.dot_general(
            p_ref[...], x_ref[...], (((1,), (1,)), ((), ())), preferred_element_type=jnp.float32
        )
        turned = turned.astype(jnp.bfloat16).reshape(4, 64, count)
        sx, sz = pl.program_id(0) // 4, pl.program_id(0) % 4
        yk[:, 0, 0] = turned[:2]
        ys[:, 0, 0] = turned[2:]
        for i in (0, 1):
            pyk[i, 0, 0] = turned[2 * i]
            pys[i, 0, 0] = turned[2 * i + 1]

        def put(ref, at, swapped):
            for s in range(4):
                if at == "x":
                    ref[0, s, 0] = turned[mirrored(s) if swapped else s]
                else:
                    ref[0, 0, s] = turned[mirrored(s) if swapped else s]

        for s, at, kept, sent, pkept, psent in ((sx, "x", xk, xs, pxk, pxs), (sz, "z", zk, zs, pzk, pzs)):
            pl.when(s < 2)(lambda: put(kept, at, False))
            pl.when(s >= 2)(lambda: put(sent, at, False))
            pl.when(s % 2 == 0)(lambda: put(pkept, at, True))
            pl.when(s % 2 == 1)(lambda: put(psent, at, True))

    def source(g, place):
        x, z = place[g // 4], place[4 + g % 4]
        return (0, (x // 2) * 8 + z * 2 + x % 2)

    def x_kept(g, place):
        g = jnp.minimum(g, 7)
        return (g // 4, 0, g % 4, 0, 0)

    def x_sent(g, place):
        g = jnp.maximum(g, 8) - 8
        return (g // 4, 0, g % 4, 0, 0)

    def x_pkept(g, place):
        return (g // 8, 0, jnp.where((g // 4) % 2 == 0, mirrored(g % 4), 3), 0, 0)

    def x_psent(g, place):
        live = (g // 4) % 2 == 1
        return (
            jnp.where(g < 12, 0, 1),
            0,
            jnp.where(live, mirrored(g % 4), jnp.where(g < 4, 0, 3)),
            0,
            0,
        )

    def y_own(g, place):
        return (0, g % 4, g // 4, 0, 0)

    def y_other(g, place):
        return (0, mirrored(g % 4), mirrored(g // 4), 0, 0)

    def z_kept(g, place):
        return (jnp.minimum(g % 4, 1), g // 4, 0, 0, 0)

    def z_sent(g, place):
        last = jnp.maximum(g // 4 * 4 + jnp.where(g % 4 < 2, -1, g % 4), 2)
        return (last % 4 - 2, last // 4, 0, 0, 0)

    def z_pkept(g, place):
        return (g % 4 // 2, mirrored(g // 4), 0, 0, 0)

    def z_psent(g, place):
        last = jnp.maximum(g // 4 * 4 + jnp.where(g % 4 == 0, -1, g % 4), 1)
        return (jnp.where(last % 4 == 3, 1, 0), mirrored(last // 4), 0, 0, 0)

    blocks = {"x": (1, 4, 1, 64, count), "y": (2, 1, 1, 64, count), "z": (1, 1, 4, 64, count)}
    maps = {
        "x": (x_kept, x_sent, x_pkept, x_psent),
        "y": (y_own, y_own, y_other, y_other),
        "z": (z_kept, z_sent, z_pkept, z_psent),
    }
    shape = jax.ShapeDtypeStruct((2, 4, 4, 64, count), jnp.bfloat16)
    return pl.pallas_call(
        kernel,
        grid_spec=pltpu.PrefetchScalarGridSpec(
            num_scalar_prefetch=1,
            grid=(16,),
            in_specs=[
                pl.BlockSpec((count, 256), source),
                pl.BlockSpec((256, 256), lambda g, place: (0, 0)),
            ],
            out_specs=[pl.BlockSpec(blocks[a], m) for a in "xyz" for m in maps[a]],
        ),
        out_shape=[shape] * 12,
        cost_estimate=pl.CostEstimate(
            flops=6_000_000_000, bytes_accessed=14 * count * D, transcendentals=0
        ),
        name="laid_out",
    )(places, tokens_in, shuffle)


def finished(sent, kept, axis):
    first = swap(sent, axis, 0)
    second = swap(narrow(wide(kept[1]) + wide(first[1])), axis, 1)
    return wide(kept[0]) + wide(first[0]) + wide(second)


def shards(
    tokens_in, query_cotangent, task_index, loss_weights, master, moment_first, moment_second
):
    xh, z, xl, y, core = (lax.axis_index(a) for a in AXES)
    near = 1 + 2 * core
    order = jnp.stack([0 * near, 4 - near, near, 0 * near + 2])
    rows = lax.iota(jnp.int32, 256)
    wanted = jnp.repeat(order ^ y, 64) * 64 + rows % 64
    shuffle = (wanted[:, None] == rows[None, :]).astype(jnp.bfloat16)
    turned = laid_out(tokens_in, jnp.concatenate([order ^ (2 * xh + xl), order ^ z]), shuffle)
    labels = lax.iota(jnp.int32, loss_weights.shape[0])
    member = task_index[:, None] == labels[None, :]
    local_counts = jnp.sum(member.astype(jnp.int32), axis=0)
    counts = total(jnp.pad(local_counts, (0, 112))[None])[0, :16]
    task_scale = loss_weights.astype(jnp.float32) / counts.astype(jnp.float32)
    task_scale = task_scale * DOWN
    token_scale = jnp.sum(jnp.where(member, task_scale[None, :], jnp.float32(0.0)), axis=1)

    def weighted(which, begin, width):
        part = lax.dynamic_slice(
            query_cotangent, (0, which * HALF + begin), (query_cotangent.shape[0], width)
        )
        return (part.astype(jnp.float32) * token_scale[:, None]).astype(jnp.bfloat16)

    parts = range(len(WIDTHS))
    starts = [sum(WIDTHS[:k]) for k in parts]
    other = [weighted(1 - core, starts[k], WIDTHS[k]) for k in parts]
    own = [weighted(core, starts[k], WIDTHS[k]) for k in parts]
    other, own = lax.optimization_barrier((other, own))

    def product(rows, weights):
        flat = rows.reshape(-1, rows.shape[-1])
        return lax.dot_general(
            flat, weights, (((1,), (0,)), ((), ())), preferred_element_type=jnp.float32
        )

    def pair(side, k):
        rows = turned[4 * "xyz".index(ORDERS[k][0]) + side]
        theirs_rows = turned[4 * "xyz".index(ORDERS[k][0]) + 2 + side]
        theirs = swap(narrow(product(theirs_rows, other[k])), "c", 0)
        out = narrow(product(rows, own[k]) + wide(theirs))
        return lax.optimization_barrier(out).reshape(2, 4, 4, 64, WIDTHS[k])

    sent = [pair(1, k) for k in parts]
    kept = [pair(0, k) for k in parts]
    for step in range(3):
        sums = [finished(sent[k], kept[k], ORDERS[k][step]) for k in parts]
        if step < 2:
            sums = [narrow(value) for value in sums]
            sent, kept = [v[2:] for v in sums], [v[:2] for v in sums]
    final = jnp.concatenate(sums, axis=-1) * UP
    square_sum = jnp.sum(final * final)
    square_sum = total(jnp.broadcast_to(square_sum, (1, 128)))[0, 0]
    final = final.reshape(2, 32, HALF)
    here = lax.dynamic_index_in_dim(final, core, 0, keepdims=False)
    theirs = lax.dynamic_index_in_dim(final, 1 - core, 0, keepdims=False)
    theirs = swap(theirs, "c", 0)
    gradient = jnp.concatenate(
        [jnp.where(core == 0, here, theirs), jnp.where(core == 0, theirs, here)], axis=1
    )
    root_mean = jnp.sqrt(square_sum / (D * QW))
    factor = 1.0 / jnp.maximum(root_mean, 1.0)
    clipped = gradient * factor
    new_first = beta_one * moment_first + (1.0 - beta_one) * clipped
    new_second = beta_two * moment_second + (1.0 - beta_two) * clipped * clipped
    direction = new_first / corr_one / (jnp.sqrt(new_second / corr_two) + adam_eps)
    new_master = master - step_rate * (direction + decay_rate * master)
    return (new_master, new_first, new_second)


def solution(mesh):
    finer = Mesh(mesh.devices.reshape(SIZES), AXES)
    rows = P(AXES, None)
    in_specs = (rows, rows, P(AXES), P(), rows, rows, rows)
    return jax.shard_map(
        shards, mesh=finer, in_specs=in_specs, out_specs=(rows, rows, rows), check_vma=False
    )
```

```python
import jax
import jax.numpy as jnp
from jax import lax
from jax.experimental import pallas as pl
from jax.experimental.pallas import tpu as pltpu
from jax.sharding import Mesh
from jax.sharding import PartitionSpec as P

D = 4096
QW = 2048
AXES = ("task_0", "task_1", "dp_0", "dp_1", "dp_2")
SIZES = (2, 4, 2, 4, 2)
DEVICES = 128
DOWN = 2.0**-11
UP = 2.0**11
HALF = QW // 2
WIDTH = 256
STARTS = (0, 512, 256, 768)


beta_one = 0.9
beta_two = 0.95
adam_eps = 1e-08
step_rate = 0.01
decay_rate = 0.1
corr_one = 1.0 - 0.9**10
corr_two = 1.0 - 0.95**10


def coords(index):
    out = []
    for size in reversed(SIZES):
        out.append(index % size)
        index //= size
    return out[::-1]


def number(parts):
    index = 0
    for part, size in zip(parts, SIZES):
        index = index * size + part
    return index


def flipped(parts, axis, both):
    xh, z, xl, y, c = parts
    if axis == "x":
        return (xh ^ both, z, xl ^ 1, y, c)
    if axis == "y":
        return (xh, z, xl, y ^ (1 + 2 * both), c)
    if axis == "z":
        return (xh, z ^ (1 + 2 * both), xl, y, c)
    return (xh, z, xl, y, c ^ 1)


def swap(value, axis, step):
    pairs = []
    for index in range(DEVICES):
        parts = coords(index)
        if step == 2:
            far = flipped(flipped(parts, axis, 0), axis, 1)
        else:
            far = flipped(parts, axis, parts[4] ^ step)
        pairs.append((index, number(far)))
    return lax.ppermute(value, AXES, pairs)


def wide(value):
    return value.astype(jnp.float32)


def narrow(value):
    return value.astype(jnp.float16)


def total(value):
    spread = jnp.broadcast_to(value[None], (DEVICES, 1, 128))
    arrived = lax.all_to_all(spread, AXES, split_axis=0, concat_axis=0, tiled=True)
    return arrived.sum(axis=0)


def mirrored(s):
    return (s % 2) * 2 + s // 2


def laid_out(tokens_in, places, shuffle, side):
    count = tokens_in.shape[0]

    def at(i):
        return slice(0, 1) if side else pl.ds(i, 1)

    def kernel(place, x0, x1, x2, x3, p_ref, x_own, x_other, y_own, y_other):
        sx = pl.program_id(0)
        for z, x_ref in enumerate((x0, x1, x2, x3)):
            turned = lax.dot_general(
                p_ref[...], x_ref[...], (((1,), (1,)), ((), ())), preferred_element_type=jnp.float32
            )
            turned = turned.astype(jnp.bfloat16).reshape(4, 64, count)
            for i in (0, 1):
                y_own[i, at(sx), z] = turned[2 * side + i][None]
                y_other[i, at(mirrored(sx)), mirrored(z)] = turned[2 * i + side][None]

            def put_own(z=z, turned=turned):
                for s in range(4):
                    x_own[at(sx % 2), s, z] = turned[s][None]

            def put_other(z=z, turned=turned):
                for s in range(4):
                    x_other[at(sx // 2), mirrored(s), mirrored(z)] = turned[s][None]

            pl.when(sx // 2 == side)(put_own)
            pl.when(sx % 2 == side)(put_other)

    def source(z):
        def index(g, place):
            x = place[g]
            return (0, (x // 2) * 8 + place[4 + z] * 2 + x % 2)

        return pl.BlockSpec((count, 256), index)

    def x_own_at(g, place):
        return (jnp.maximum(g, 2) - 2, 0, 0, 0, 0)

    def x_other_at(g, place):
        return (jnp.maximum(g - 1, 0) // 2, 0, 0, 0, 0)

    if side:
        shape = pltpu.HBM((2, 4, 4, 64, count), jnp.bfloat16)
        out_specs = [
            pl.BlockSpec((1, 4, 4, 64, count), x_own_at),
            pl.BlockSpec((1, 4, 4, 64, count), x_other_at),
            pl.BlockSpec((2, 1, 4, 64, count), lambda g, place: (0, g, 0, 0, 0)),
            pl.BlockSpec((2, 1, 4, 64, count), lambda g, place: (0, mirrored(g), 0, 0, 0)),
        ]
    else:
        shape = pltpu.VMEM((2, 4, 4, 64, count), jnp.bfloat16)
        out_specs = [pl.BlockSpec(memory_space=pltpu.VMEM)] * 4
    return pl.pallas_call(
        kernel,
        grid_spec=pltpu.PrefetchScalarGridSpec(
            num_scalar_prefetch=1,
            grid=(4,),
            in_specs=[
                *(source(z) for z in range(4)),
                pl.BlockSpec((256, 256), lambda g, place: (0, 0)),
            ],
            out_specs=out_specs,
        ),
        out_shape=[shape] * 4,
        compiler_params=pltpu.CompilerParams(vmem_limit_bytes=(56 if side else 8) << 20),
        cost_estimate=pl.CostEstimate(
            flops=6_000_000_000, bytes_accessed=6 * count * D, transcendentals=0
        ),
        name="laid_out",
    )(places, tokens_in, tokens_in, tokens_in, tokens_in, shuffle)


def finished(sent, kept, axis):
    first = swap(sent, axis, 0)
    second = swap(narrow(wide(kept[1]) + wide(first[1])), axis, 1)
    return wide(kept[0]) + wide(first[0]) + wide(second)


def shards(
    tokens_in, query_cotangent, task_index, loss_weights, master, moment_first, moment_second
):
    xh, z, xl, y, core = (lax.axis_index(a) for a in AXES)
    near = 1 + 2 * core
    order = jnp.stack([0 * near, 4 - near, near, 0 * near + 2])
    rows = lax.iota(jnp.int32, 256)
    wanted = jnp.repeat(order ^ y, 64) * 64 + rows % 64
    shuffle = (wanted[:, None] == rows[None, :]).astype(jnp.bfloat16)
    places = jnp.concatenate([order ^ (2 * xh + xl), order ^ z])
    to_send = laid_out(tokens_in, places, shuffle, 1)
    labels = lax.iota(jnp.int32, loss_weights.shape[0])
    member = task_index[:, None] == labels[None, :]
    local_counts = jnp.sum(member.astype(jnp.int32), axis=0)
    counts = total(jnp.pad(local_counts, (0, 112))[None])[0, :16]
    task_scale = loss_weights.astype(jnp.float32) / counts.astype(jnp.float32)
    task_scale = task_scale * DOWN
    token_scale = jnp.sum(jnp.where(member, task_scale[None, :], jnp.float32(0.0)), axis=1)

    def weighted(which, begin, width):
        part = lax.dynamic_slice(
            query_cotangent, (0, which * HALF + begin), (query_cotangent.shape[0], width)
        )
        return (part.astype(jnp.float32) * token_scale[:, None]).astype(jnp.bfloat16)

    parts = range(4)
    other = [weighted(1 - core, STARTS[k], WIDTH) for k in parts]
    own = [weighted(core, STARTS[k], WIDTH) for k in parts]
    other, own = lax.optimization_barrier((other, own))

    def product(rows, weights):
        flat = rows.reshape(-1, rows.shape[-1])
        return lax.dot_general(
            flat, weights, (((1,), (0,)), ((), ())), preferred_element_type=jnp.float32
        )

    def pairs(turned):
        outs = []
        for k in parts:
            theirs = swap(narrow(product(turned[2 * (k % 2) + 1], other[k])), "c", 0)
            out = narrow(product(turned[2 * (k % 2)], own[k]) + wide(theirs))
            outs.append(lax.optimization_barrier(out).reshape(2, 4, 4, 64, WIDTH))
        return outs

    sent = pairs(to_send)
    to_keep = laid_out(tokens_in, places, shuffle, 0)
    kept = pairs(to_keep)
    sums = [narrow(finished(sent[k], kept[k], "xy"[k % 2])) for k in parts]
    sums = [jnp.concatenate([sums[k], sums[k + 2]], axis=-1) for k in (0, 1)]
    sums = [narrow(finished(v[2:], v[:2], "yx"[k])) for k, v in enumerate(sums)]
    both = jnp.concatenate(sums, axis=-1)
    final = wide(both[0])
    for slot, step in ((1, 1), (2, 0), (3, 2)):
        final = final + wide(swap(both[slot], "z", step))
    final = final * UP
    square_sum = jnp.sum(final * final)
    square_sum = total(jnp.broadcast_to(square_sum, (1, 128)))[0, 0]
    final = final.reshape(2, 32, HALF)
    here = lax.dynamic_index_in_dim(final, core, 0, keepdims=False)
    theirs = lax.dynamic_index_in_dim(final, 1 - core, 0, keepdims=False)
    theirs = swap(theirs, "c", 0)
    gradient = jnp.concatenate(
        [jnp.where(core == 0, here, theirs), jnp.where(core == 0, theirs, here)], axis=1
    )
    root_mean = jnp.sqrt(square_sum / (D * QW))
    factor = 1.0 / jnp.maximum(root_mean, 1.0)
    clipped = gradient * factor
    new_first = beta_one * moment_first + (1.0 - beta_one) * clipped
    new_second = beta_two * moment_second + (1.0 - beta_two) * clipped * clipped
    direction = new_first / corr_one / (jnp.sqrt(new_second / corr_two) + adam_eps)
    new_master = master - step_rate * (direction + decay_rate * master)
    return (new_master, new_first, new_second)


def solution(mesh):
    finer = Mesh(mesh.devices.reshape(SIZES), AXES)
    rows = P(AXES, None)
    in_specs = (rows, rows, P(AXES), P(), rows, rows, rows)
    return jax.shard_map(shards, mesh=finer, in_specs=in_specs, out_specs=(rows, rows, rows), check_vma=False)
```

```python
import jax
import jax.numpy as jnp
from jax import lax
from jax.experimental import pallas as pl
from jax.experimental.pallas import tpu as pltpu
from jax.sharding import Mesh
from jax.sharding import PartitionSpec as P

D = 4096
QW = 2048
AXES = ("task_0", "task_1", "dp_0", "dp_1", "dp_2")
SIZES = (2, 4, 2, 4, 2)
DEVICES = 128
DOWN = 2.0**-11
UP = 2.0**11
HALF = QW // 2
WIDTH = 256
STARTS = (0, 512, 256, 768)


beta_one = 0.9
beta_two = 0.95
adam_eps = 1e-08
step_rate = 0.01
decay_rate = 0.1
corr_one = 1.0 - 0.9**10
corr_two = 1.0 - 0.95**10


def coords(index):
    out = []
    for size in reversed(SIZES):
        out.append(index % size)
        index //= size
    return out[::-1]


def number(parts):
    index = 0
    for part, size in zip(parts, SIZES):
        index = index * size + part
    return index


def flipped(parts, axis, both):
    xh, z, xl, y, c = parts
    if axis == "x":
        return (xh ^ both, z, xl ^ 1, y, c)
    if axis == "y":
        return (xh, z, xl, y ^ (1 + 2 * both), c)
    if axis == "z":
        return (xh, z ^ (1 + 2 * both), xl, y, c)
    return (xh, z, xl, y, c ^ 1)


def swap(value, axis, step):
    pairs = []
    for index in range(DEVICES):
        parts = coords(index)
        if step == 2:
            far = flipped(flipped(parts, axis, 0), axis, 1)
        else:
            far = flipped(parts, axis, parts[4] ^ step)
        pairs.append((index, number(far)))
    return lax.ppermute(value, AXES, pairs)


def wide(value):
    return value.astype(jnp.float32)


def narrow(value):
    return value.astype(jnp.float16)


def total(value):
    spread = jnp.broadcast_to(value[None], (DEVICES, 1, 128))
    arrived = lax.all_to_all(spread, AXES, split_axis=0, concat_axis=0, tiled=True)
    return arrived.sum(axis=0)


def mirrored(s):
    return (s % 2) * 2 + s // 2


def laid_out(tokens_in, places, shuffle):
    count = tokens_in.shape[0]

    def kernel(place, x0, x1, x2, x3, p_ref, *refs):
        sx = pl.program_id(0)
        for z, x_ref in enumerate((x0, x1, x2, x3)):
            turned = lax.dot_general(
                p_ref[...], x_ref[...], (((1,), (1,)), ((), ())), preferred_element_type=jnp.float32
            )
            turned = turned.astype(jnp.bfloat16).reshape(4, 64, count)
            for side in (0, 1):
                x_own, x_other, y_own, y_other = refs[4 * side : 4 * side + 4]
                for i in (0, 1):
                    y_own[i, 0, z] = turned[2 * side + i]
                    y_other[i, 0, mirrored(z)] = turned[2 * i + side]

                def put_own(z=z, turned=turned, x_own=x_own):
                    x_own[0, :, z] = turned

                def put_other(z=z, turned=turned, x_other=x_other):
                    for s in range(4):
                        x_other[0, mirrored(s), mirrored(z)] = turned[s]

                pl.when(sx // 2 == side)(put_own)
                pl.when(sx % 2 == side)(put_other)

    def source(z):
        def index(g, place):
            x = place[g]
            return (0, (x // 2) * 8 + place[4 + z] * 2 + x % 2)

        return pl.BlockSpec((count, 256), index)

    first = (
        (lambda g, place: (jnp.minimum(g, 1), 0, 0, 0, 0), lambda g, place: (g // 2, 0, 0, 0, 0)),
        (
            lambda g, place: (jnp.maximum(g, 2) - 2, 0, 0, 0, 0),
            lambda g, place: (jnp.maximum(g - 1, 0) // 2, 0, 0, 0, 0),
        ),
    )
    out_specs = []
    for side in (0, 1):
        out_specs += [pl.BlockSpec((1, 4, 4, 64, count), index) for index in first[side]]
        out_specs += [
            pl.BlockSpec((2, 1, 4, 64, count), lambda g, place: (0, g, 0, 0, 0)),
            pl.BlockSpec((2, 1, 4, 64, count), lambda g, place: (0, mirrored(g), 0, 0, 0)),
        ]
    return pl.pallas_call(
        kernel,
        grid_spec=pltpu.PrefetchScalarGridSpec(
            num_scalar_prefetch=1,
            grid=(4,),
            in_specs=[
                *(source(z) for z in range(4)),
                pl.BlockSpec((256, 256), lambda g, place: (0, 0)),
            ],
            out_specs=out_specs,
        ),
        out_shape=[pltpu.HBM((2, 4, 4, 64, count), jnp.bfloat16)] * 8,
        compiler_params=pltpu.CompilerParams(vmem_limit_bytes=56 << 20),
        cost_estimate=pl.CostEstimate(
            flops=6_000_000_000, bytes_accessed=10 * count * D, transcendentals=0
        ),
        name="laid_out",
    )(places, tokens_in, tokens_in, tokens_in, tokens_in, shuffle)


def finished(sent, kept, axis):
    first = swap(sent, axis, 0)
    second = swap(narrow(wide(kept[1]) + wide(first[1])), axis, 1)
    return narrow(wide(kept[0]) + wide(first[0]) + wide(second))


def shards(
    tokens_in, query_cotangent, task_index, loss_weights, master, moment_first, moment_second
):
    xh, z, xl, y, core = (lax.axis_index(a) for a in AXES)
    near = 1 + 2 * core
    order = jnp.stack([0 * near, 4 - near, near, 0 * near + 2])
    rows = lax.iota(jnp.int32, 256)
    wanted = jnp.repeat(order ^ y, 64) * 64 + rows % 64
    shuffle = (wanted[:, None] == rows[None, :]).astype(jnp.bfloat16)
    places = jnp.concatenate([order ^ (2 * xh + xl), order ^ z])
    turned = laid_out(tokens_in, places, shuffle)
    to_keep, to_send = turned[:4], turned[4:]
    labels = lax.iota(jnp.int32, loss_weights.shape[0])
    member = task_index[:, None] == labels[None, :]
    local_counts = jnp.sum(member.astype(jnp.int32), axis=0)
    counts = total(jnp.pad(local_counts, (0, 112))[None])[0, :16]
    task_scale = loss_weights.astype(jnp.float32) / counts.astype(jnp.float32)
    task_scale = task_scale * DOWN
    token_scale = jnp.sum(jnp.where(member, task_scale[None, :], jnp.float32(0.0)), axis=1)

    def weighted(which, begin, width):
        part = lax.dynamic_slice(
            query_cotangent, (0, which * HALF + begin), (query_cotangent.shape[0], width)
        )
        return (part.astype(jnp.float32) * token_scale[:, None]).astype(jnp.bfloat16)

    parts = range(4)
    other, own = [], []
    for half in (0, 1):
        these = lax.optimization_barrier(
            [weighted(c, STARTS[2 * half + k], WIDTH) for c in (1 - core, core) for k in (0, 1)]
        )
        other += these[:2]
        own += these[2:]

    def product(rows, weights):
        flat = rows.reshape(-1, rows.shape[-1])
        return lax.dot_general(
            flat, weights, (((1,), (0,)), ((), ())), preferred_element_type=jnp.float32
        )

    def pairs(turned):
        outs = []
        for k in parts:
            theirs = narrow(product(turned[2 * (k % 2) + 1], other[k]))
            theirs = swap(theirs, "c", 0)
            out = narrow(product(turned[2 * (k % 2)], own[k]) + wide(theirs))
            outs.append(lax.optimization_barrier(out).reshape(2, 4, 4, 64, WIDTH))
        return outs

    sent = pairs(to_send)
    kept = pairs(to_keep)
    sums = [finished(sent[k], kept[k], "xy"[k % 2]) for k in parts]
    sums = [jnp.concatenate([sums[k], sums[k + 2]], axis=-1) for k in (0, 1)]
    sums = [finished(v[2:], v[:2], "yx"[k]) for k, v in enumerate(sums)]
    both = jnp.concatenate(sums, axis=-1)
    final = wide(both[0])
    for slot, step in ((1, 1), (2, 0), (3, 2)):
        final = final + wide(swap(both[slot], "z", step))
    final = final * UP
    square_sum = jnp.sum(final * final)
    square_sum = total(jnp.broadcast_to(square_sum, (1, 128)))[0, 0]
    final = final.reshape(2, 32, HALF)
    here = lax.dynamic_index_in_dim(final, core, 0, keepdims=False)
    theirs = lax.dynamic_index_in_dim(final, 1 - core, 0, keepdims=False)
    theirs = swap(theirs, "c", 0)
    gradient = jnp.concatenate(
        [jnp.where(core == 0, here, theirs), jnp.where(core == 0, theirs, here)], axis=1
    )
    root_mean = jnp.sqrt(square_sum / (D * QW))
    factor = 1.0 / jnp.maximum(root_mean, 1.0)
    clipped = gradient * factor
    new_first = beta_one * moment_first + (1.0 - beta_one) * clipped
    new_second = beta_two * moment_second + (1.0 - beta_two) * clipped * clipped
    direction = new_first / corr_one / (jnp.sqrt(new_second / corr_two) + adam_eps)
    new_master = master - step_rate * (direction + decay_rate * master)
    return (new_master, new_first, new_second)


def solution(mesh):
    finer = Mesh(mesh.devices.reshape(SIZES), AXES)
    rows = P(AXES, None)
    in_specs = (rows, rows, P(AXES), P(), rows, rows, rows)
    return jax.shard_map(shards, mesh=finer, in_specs=in_specs, out_specs=(rows, rows, rows), check_vma=False)
```
